512 devices in a mesh: chip: 32 (over x_hi, y, core), line: 16 (over z, x_lo).
Axes of the slice: x: 4 (x_hi: 2, x_lo: 2; x = x_hi * 2 + x_lo), y: 8, z: 8, core: 2. Of those that a mesh axis runs over, the one named last changes fastest.
Arguments:
- echoes: bfloat16 [32, 2, 4096, 4096], P('chip', None, 'line'), may hold values from -6 to 6
- range_filter: float32 [2, 4096], replicated, may hold values from -6 to 6
- rcmc_weights: float32 [8, 4096], replicated, may hold values from -3 to 3
- fm_rate: float32 [32, 384], P('chip', 'line'), may hold values from 256 to 2048
- rcmc_shift: int32 [32, 384], P('chip', 'line'), may hold values from 0 to 12, as said below
- seam_width: int32 [32], P('chip'), may hold values from 64 to 128, as said below
- seam_link: int32 [32], P('chip'), may hold values from 0 to 1
Outputs:
- image: bfloat16 [32, 2, 384, 4096], P('chip', None, 'line')
The draws below stay inside these ranges and needn't reach their ends.
Inputs may be any that keep to these rules, and one draw needn't show every extreme that they name: `rcmc_shift`: every draw has some entry equal to 12. `seam_width`: every draw has some chip with the width 128.
All inputs are finite; a program needn't handle non-finite values.
Results may differ from the reference program's by a relative error of at most 0.0011.
Values sent between devices are 32-bit elements; how exact they have to be, the bound alone decides.
A program may use at most 64 MiB of HBM per device.

```python
import math
import jax
import jax.numpy as jnp
from jax import lax

AZ = 4096
RG = 4096
RKEEP = 384
TAPS = 8
MAXSHIFT = 12
OVL = 128
CHIPS = 32


def draw_rcmc_shift(key, part):
    first, second = jax.random.split(jax.random.fold_in(key, 11))
    values = jax.random.randint(first, (CHIPS, RKEEP), 0, MAXSHIFT + 1, dtype=jnp.int32)
    where_max = jax.random.randint(second, (), 0, CHIPS * RKEEP, dtype=jnp.int32)
    flattened = values.reshape(-1).at[where_max].set(MAXSHIFT)
    return flattened.reshape(CHIPS, RKEEP)


def draw_seam_width(key, part):
    first, second = jax.random.split(jax.random.fold_in(key, 23))
    values = jax.random.randint(first, (CHIPS,), OVL // 2, OVL + 1, dtype=jnp.int32)
    where_max = jax.random.randint(second, (), 0, CHIPS, dtype=jnp.int32)
    return values.at[where_max].set(OVL)


def draw_seam_link(key, part):
    values = jax.random.randint(jax.random.fold_in(key, 37), (CHIPS,), 0, 4, dtype=jnp.int32)
    linked = (values > 0).astype(jnp.int32)
    return linked.at[0].set(0)


def shard_levels(rng, shape, pieces, smallest, high):
    factor_of, own = 1.0, jax.random.fold_in(rng, 6)
    for axis_at, shards_of in pieces:
        steps = jnp.exp(jax.random.uniform(jax.random.fold_in(own, axis_at), (shards_of,), jnp.float32, smallest / len(pieces), high / len(pieces)))
        factor_of = factor_of * jnp.repeat(steps, shape[axis_at] // shards_of).reshape([-1 if axis == axis_at else 1 for axis in range(len(shape))])
    return factor_of


def noise(own_key, extent, deviation, reach, pieces=(), kind=jnp.bfloat16):
    level = shard_levels(own_key, extent, pieces, -0.22, 0.18) if pieces else 1.0
    entries = jax.random.normal(own_key, extent, jnp.float32) * deviation * level
    return jnp.minimum(jnp.maximum(entries, -reach), reach).astype(kind)


def setup_inputs(seed: int = 0) -> dict:
    key_list = jax.random.split(jax.random.key(seed), 8)
    echoes = noise(key_list[0], (CHIPS, 2, AZ, RG), 1.0, 6.0, ((0, 32), (2, 16)))
    range_filter = noise(key_list[1], (2, RG), 1.0, 6.0, (), jnp.float32)
    rcmc_weights = noise(key_list[2], (TAPS, AZ), 0.5, 3.0, (), jnp.float32)
    fm_rate = jnp.clip(jnp.exp(math.log(2048.0) - 2.0794415 * jax.random.uniform(key_list[3], (CHIPS, RKEEP), jnp.float32) ** shard_levels(key_list[3], (CHIPS, RKEEP), ((0, 32), (1, 16)), -0.2, 0.2)), 256.0, 2048.0)
    rcmc_shift = draw_rcmc_shift(jax.random.fold_in(key_list[7], 71), 0)
    seam_width = draw_seam_width(jax.random.fold_in(key_list[7], 71), 0)
    seam_link = draw_seam_link(jax.random.fold_in(key_list[7], 71), 0)
    return {"echoes": echoes, "range_filter": range_filter, "rcmc_weights": rcmc_weights, "fm_rate": fm_rate, "rcmc_shift": rcmc_shift, "seam_width": seam_width, "seam_link": seam_link}


def reference(echoes, range_filter, rcmc_weights, fm_rate, rcmc_shift, seam_width, seam_link):
    margin = MAXSHIFT + TAPS - 1
    filter_pair = lax.complex(range_filter[0], range_filter[1])

    def focus_chip(inputs):
        echo, rate, shift = inputs
        raw = lax.complex(echo[0].astype(jnp.float32), echo[1].astype(jnp.float32))
        compressed = jnp.fft.ifft(jnp.fft.fft(raw, axis=1) * filter_pair[None], axis=1)[:, :RKEEP]
        gain = 1.0 + 2.0 * jnp.arange(RKEEP, dtype=jnp.float32) / RKEEP
        compressed = compressed * gain[None]
        doppler = jnp.fft.fft(compressed, axis=0).T
        padded = jnp.concatenate([doppler, jnp.zeros((margin, AZ), doppler.dtype)], axis=0)
        positions = jnp.arange(RKEEP, dtype=jnp.int32) + shift
        migrated = jnp.zeros((RKEEP, AZ), doppler.dtype)
        for offset in range(TAPS):
            migrated = migrated + rcmc_weights[offset][None] * jnp.take(padded, positions + offset, axis=0)
        index = jnp.arange(AZ, dtype=jnp.int32)
        frequency = ((index + AZ // 2) % AZ - AZ // 2).astype(jnp.float32) / AZ
        phase = math.pi * (rate[:, None] * (frequency * frequency)[None, :])
        filtered = migrated * lax.complex(jnp.cos(phase), -jnp.sin(phase))
        focused = jnp.fft.ifft(filtered, axis=1)
        return jnp.stack([jnp.real(focused), jnp.imag(focused)])
    focused = lax.map(focus_chip, (echoes, fm_rate, rcmc_shift))
    tails = jnp.concatenate([jnp.zeros((1, 2, RKEEP, OVL), focused.dtype), focused[:-1, :, :, AZ - OVL:]], axis=0)
    offsets = jnp.arange(OVL, dtype=jnp.int32)
    columns = jnp.clip(OVL - seam_width[:, None] + offsets[None], 0, OVL - 1)
    previous = jax.vmap(lambda tail_block, column: jnp.take(tail_block, column, axis=2))(tails, columns)
    ramp = (offsets.astype(jnp.float32)[None] + 0.5) / seam_width[:, None].astype(jnp.float32)
    inside = (offsets[None] < seam_width[:, None]) & (seam_link[:, None] == 1)
    ramp = ramp[:, None, None, :]
    inside = inside[:, None, None, :]
    head = focused[:, :, :, :OVL]
    mixed = jnp.where(inside, (1.0 - ramp) * previous + ramp * head, head)
    blended = jnp.concatenate([mixed, focused[:, :, :, OVL:]], axis=3)
    energy = lax.optimization_barrier(jnp.sum(blended * blended, axis=(1, 2, 3)))
    scale = lax.rsqrt(energy / (RKEEP * AZ) + 1e-06)
    return (blended * scale[:, None, None, None]).astype(jnp.bfloat16)
```

```python
import math

import jax
import jax.numpy as jnp
import numpy as np
from jax import lax
from jax.experimental import pallas as pl
from jax.experimental.pallas import tpu as pltpu
from jax.sharding import PartitionSpec as P

F32 = jnp.float32
BF16 = jnp.bfloat16
AZ = 4096
RKEEP = 384
TAPS = 8
OVL = 128
LINES = 16
ROWS = RKEEP // LINES
NEED = 44
SLOT = 104
HIGHEST = lax.Precision.HIGHEST
MESH = pl.DeviceIdType.MESH


def place(comp, i):
    if i < 16:
        return comp * 16 + i
    if i < 20:
        return 32 + comp * 4 + i - 16
    return 40 + comp * 4 + i - 20


def split(value):
    high = value.astype(BF16)
    return high, (value - high.astype(F32)).astype(BF16)


def angles(rows, columns, length, sign):
    product = np.outer(np.asarray(rows, np.int64), np.asarray(columns, np.int64)) % length
    theta = sign * 2.0 * np.pi / length * product
    return np.cos(theta), np.sin(theta)


def split_table(table, axis):
    import ml_dtypes

    high = table.astype(np.float32).astype(ml_dtypes.bfloat16)
    low = (table - high.astype(np.float64)).astype(np.float32).astype(ml_dtypes.bfloat16)
    return np.concatenate([high, high, low], axis=axis)


def tables():
    n32, n128 = np.arange(32), np.arange(128)
    c, s = angles(n32, n32, 32, -1)
    first = np.block([[c, -s], [s, c]])
    filter_turn = np.stack(angles(n32, n128, 4096, -1))
    shift = (4 * n32[None, :] - np.arange(4)[:, None]).reshape(-1)
    c, s = angles(shift, n128, 128, 1)
    second = np.block([[c, -s], [s, c]]) / 4096.0
    c, s = angles(n32, n32, 32, -1)
    forward32 = np.block([[c, -s], [s, c]])
    turn = np.stack(angles(n32, n128, 4096, -1))
    c, s = angles(n128, n128, 128, -1)
    forward128 = np.block([[c, s], [-s, c]])
    c, s = angles(n128, n128, 128, 1)
    inverse128 = np.block([[c, s], [-s, c]])
    c, s = angles(n32, n32, 32, 1)
    inverse32 = np.block([[c, -s], [s, c]]) / 4096.0
    f32 = lambda t: t.astype(np.float32)
    return (
        f32(first),
        f32(filter_turn),
        f32(second),
        split_table(forward32, 1),
        f32(turn),
        split_table(forward128, 0),
        split_table(inverse128, 0),
        split_table(inverse32, 1),
    )


def mm(a, b, precision=None):
    return lax.dot_general(
        a, b, (((1,), (0,)), ((), ())), precision=precision, preferred_element_type=F32
    )


def mm_nt(a, b, precision=None):
    return lax.dot_general(
        a, b, (((1,), (1,)), ((), ())), precision=precision, preferred_element_type=F32
    )


def turned(real, imag, c, s):
    return real * c - imag * s, real * s + imag * c


def kernel(
    chips,
    echo_hbm,
    filter_ref,
    weight_ref,
    rate_ref,
    shift_ref,
    width_ref,
    link_ref,
    first_ref,
    fturn_ref,
    second_ref,
    fwd32_ref,
    turn_ref,
    fwd128_ref,
    inv128_ref,
    inv32_ref,
    out_ref,
    echo,
    spectrum,
    pulse,
    band,
    acc,
    piece,
    recv,
    mid_hi,
    mid_lo,
    ext,
    cosine,
    sine,
    foc_hi,
    foc_lo,
    back,
    img,
    tail,
    tail_in,
    esend,
    erecv,
    load_sem,
    send_sem,
    recv_sem,
    fsend_sem,
    frecv_sem,
    tail_sem,
    esend_sem,
    erecv_sem,
):
    me = lax.axis_index("line")
    chip = lax.axis_index("chip")
    following = lax.rem(chip + 1, chips)
    preceding = lax.rem(chip + chips - 1, chips)
    below = lax.rem(me + LINES - 1, LINES)
    barrier = pltpu.get_barrier_semaphore()

    @pl.loop(1, LINES)
    def _(k):
        pl.semaphore_signal(
            barrier, inc=1, device_id={"line": lax.rem(me + k, LINES)}, device_id_type=MESH
        )

    pl.semaphore_signal(barrier, inc=1, device_id={"chip": following}, device_id_type=MESH)
    pl.semaphore_signal(barrier, inc=1, device_id={"chip": preceding}, device_id_type=MESH)

    def load(c):
        return pltpu.make_async_copy(
            echo_hbm.at[0, :, pl.ds(128 * c, 128), :],
            echo.at[:, pl.ds(128 * c, 128), :],
            load_sem.at[c],
        )

    load(0).start()
    load(1).start()

    for comp in range(2):
        for a in range(32):
            spectrum[pl.ds(comp * 32 + a, 1), :] = filter_ref[comp : comp + 1, 128 * a : 128 * a + 128]
    y = mm(first_ref[...], spectrum[...], HIGHEST)
    yr, yi = turned(y[:32], y[32:], fturn_ref[0], fturn_ref[1])
    y = mm_nt(second_ref[...], jnp.concatenate([yr, yi], axis=1), HIGHEST)
    for comp in range(2):
        rows = jnp.concatenate(
            [y[128 * comp + 32 * u : 128 * comp + 32 * u + 32] for u in range(4)], axis=1
        )
        pulse[pl.ds(40 * comp, 32), :] = rows
        pulse[pl.ds(40 * comp + 32, 8), :] = rows[:8]

    keep = lax.broadcasted_iota(jnp.int32, (128, 128), 1) >= lax.broadcasted_iota(
        jnp.int32, (128, 128), 0
    )

    def slanted(comp, m):
        row = pulse[pl.ds(40 * comp + m, 1), :]
        return pltpu.roll(
            jnp.broadcast_to(row, (128, 128)), 0, axis=1, stride=1, stride_axis=0
        )

    def build(m, carry):
        new = []
        at = pl.multiple_of(128 * m, 128)
        for comp in range(2):
            ahead = slanted(comp, m + 1)
            high, low = split(jnp.where(keep, carry[comp], ahead))
            band[2 * comp, pl.ds(at, 128), :] = high
            band[2 * comp + 1, pl.ds(at, 128), :] = low
            new.append(ahead)
        return tuple(new)

    lax.fori_loop(0, 34, build, (slanted(0, 0), slanted(1, 0)))

    def multiply(c):
        acc[...] = jnp.zeros_like(acc)

        @pl.loop(0, 16)
        def _(t):
            s = pl.multiple_of(256 * t, 256)
            at0 = pl.multiple_of(128 * lax.rem(32 - 2 * t, 32), 128)
            at1 = pl.multiple_of(128 * (31 - 2 * t), 128)
            xr = echo[0, 128 * c : 128 * c + 128, pl.ds(s, 256)]
            xi = echo[1, 128 * c : 128 * c + 128, pl.ds(s, 256)]
            right = jnp.concatenate(
                [
                    jnp.concatenate([xr, xr, -xi, -xi], axis=1),
                    jnp.concatenate([xi, xi, xr, xr], axis=1),
                ],
                axis=0,
            )
            left = jnp.concatenate(
                [band[part, pl.ds(at, RKEEP), :] for part in range(4) for at in (at0, at1)],
                axis=1,
            )
            acc[...] += mm_nt(left, right)

        for g in range(LINES):
            ramp = lax.broadcasted_iota(jnp.int32, (ROWS, 1), 0) + ROWS * g
            gain = 1.0 + 2.0 * ramp.astype(F32) / RKEEP
            for comp in range(2):
                v = acc[ROWS * g : ROWS * g + ROWS, 128 * comp : 128 * comp + 128] * gain
                base = 48 * g
                piece[c, base + 16 * comp : base + 16 * comp + 16, :] = v[:16]
                piece[c, base + 32 + 4 * comp : base + 36 + 4 * comp, :] = v[16:20]
                piece[c, base + 40 + 4 * comp : base + 44 + 4 * comp, :] = v[20:]

    def direct(c, k):
        to = lax.rem(me + k, LINES)
        return pltpu.make_async_remote_copy(
            src_ref=piece.at[c, pl.ds(pl.multiple_of(48 * to, 8), 48), :],
            dst_ref=recv.at[pl.ds(pl.multiple_of((2 * me + c) * SLOT, 8), 48), :],
            send_sem=send_sem.at[c, k],
            recv_sem=recv_sem.at[c, k],
            device_id={"line": to},
            device_id_type=MESH,
        )

    def onward(c, k):
        source = lax.rem(me + LINES - k, LINES)
        slot = (2 * source + c) * SLOT
        return pltpu.make_async_remote_copy(
            src_ref=recv.at[pl.ds(pl.multiple_of(slot, 8), 40), :],
            dst_ref=recv.at[pl.ds(pl.multiple_of(slot + 48, 8), 40), :],
            send_sem=fsend_sem.at[c, k],
            recv_sem=frecv_sem.at[c, k],
            device_id={"line": below},
            device_id_type=MESH,
        )

    for c in range(2):
        load(c).wait()
        multiply(c)
        if c == 0:
            pl.semaphore_wait(barrier, LINES + 1)

        @pl.loop(1, LINES)
        def _(k, c=c):
            direct(c, k).start()

        recv[pl.ds(pl.multiple_of((2 * me + c) * SLOT, 8), 48), :] = piece[
            c, pl.ds(pl.multiple_of(48 * me, 8), 48), :
        ]
        onward(c, 0).start()

    index = lax.broadcasted_iota(jnp.int32, (32, 128), 0) + 32 * lax.broadcasted_iota(
        jnp.int32, (32, 128), 1
    )
    frequency = jnp.where(index < AZ // 2, index, index - AZ).astype(F32) / AZ
    squared = frequency * frequency

    @pl.loop(0, ROWS)
    def _(r):
        turns = rate_ref[0, r] * squared
        turns = turns - 2.0 * jnp.round(turns * 0.5)
        cosine[r] = jnp.cos(math.pi * turns)
        sine[r] = jnp.sin(math.pi * turns)

    for c in range(2):

        @pl.loop(1, LINES)
        def _(k, c=c):
            direct(c, k).wait_recv()
            onward(c, k).start()

    for c in range(2):

        @pl.loop(0, LINES)
        def _(k, c=c):
            onward(c, k).wait_recv()

    tc, ts = turn_ref[0], turn_ref[1]
    last = me == LINES - 1

    def column(i):
        def part(comp):
            at = place(comp, i) if i < ROWS else 48 + place(comp, i - ROWS)
            return recv[pl.ds(at, 32, stride=SLOT), :]

        v = jnp.concatenate([part(0), part(1)], axis=0)
        return v if i < ROWS else jnp.where(last, 0.0, v)

    for i in range(0, NEED, 2):
        high, low = split(jnp.concatenate([column(i), column(i + 1)], axis=1))
        y = mm(fwd32_ref[...], jnp.concatenate([high, low, high], axis=0))
        for j in range(2):
            yr, yi = turned(y[:32, 128 * j : 128 * j + 128], y[32:, 128 * j : 128 * j + 128], tc, ts)
            high, low = split(jnp.concatenate([yr, yi], axis=1))
            mid_hi[32 * (i + j) : 32 * (i + j) + 32, :] = high
            mid_lo[32 * (i + j) : 32 * (i + j) + 32, :] = low

    @pl.loop(0, 4)
    def _(j):
        at = pl.multiple_of(352 * j, 32)
        high, low = mid_hi[pl.ds(at, 352), :], mid_lo[pl.ds(at, 352), :]
        y = mm(jnp.concatenate([high, low, high], axis=1), fwd128_ref[...])
        ext[pl.ds(11 * j, 11)] = y.reshape(11, 32, 256)

    @pl.loop(0, ROWS)
    def _(r):
        at = r + shift_ref[0, r]
        real = jnp.zeros((32, 128), F32)
        imag = jnp.zeros((32, 128), F32)
        for t in range(TAPS):
            w = weight_ref[t]
            row = ext[at + t]
            real += w * row[:, :128]
            imag += w * row[:, 128:]
        fr, fi = turned(real, imag, cosine[r], -sine[r])
        high, low = split(jnp.concatenate([fr, fi], axis=1))
        foc_hi[pl.ds(pl.multiple_of(32 * r, 32), 32), :] = high
        foc_lo[pl.ds(pl.multiple_of(32 * r, 32), 32), :] = low

    @pl.loop(0, 3)
    def _(j):
        at = pl.multiple_of(256 * j, 256)
        high, low = foc_hi[pl.ds(at, 256), :], foc_lo[pl.ds(at, 256), :]
        back[pl.ds(at, 256), :] = mm(jnp.concatenate([high, low, high], axis=1), inv128_ref[...])

    for i in range(0, ROWS, 2):
        both = []
        for j in range(2):
            v = back[32 * (i + j) : 32 * (i + j) + 32, :]
            vr, vi = turned(v[:, :128], v[:, 128:], tc, -ts)
            both.append(jnp.concatenate([vr, vi], axis=0))
        high, low = split(jnp.concatenate(both, axis=1))
        y = mm(inv32_ref[...], jnp.concatenate([high, low, high], axis=0))
        for j in range(2):
            img[64 * (i + j) : 64 * (i + j) + 64, :] = y[:, 128 * j : 128 * j + 128]

    for comp in range(2):
        tail[ROWS * comp : ROWS * comp + ROWS, :] = img[pl.ds(32 * comp + 31, ROWS, stride=64), :]
    handed = pltpu.make_async_remote_copy(
        src_ref=tail,
        dst_ref=tail_in,
        send_sem=tail_sem.at[0],
        recv_sem=tail_sem.at[1],
        device_id={"chip": following},
        device_id_type=MESH,
    )
    handed.start()

    rest = (lax.broadcasted_iota(jnp.int32, (8, 128), 0) > 0).astype(F32)

    def gather(r, total):
        v = img[pl.ds(pl.multiple_of(64 * r, 64), 64), :]
        v = v * v
        for j in range(8):
            part = v[8 * j : 8 * j + 8]
            total = total + (part * rest if j % 4 == 0 else part)
        return total

    energy = lax.fori_loop(0, ROWS, gather, jnp.zeros((8, 128), F32))

    handed.wait()
    width = width_ref[0]
    lane = lax.broadcasted_iota(jnp.int32, (1, 128), 1)
    ramp = (lane.astype(F32) + 0.5) / width.astype(F32)
    linked = (link_ref[0] == 1).astype(jnp.int32)
    inside = lane < width * linked
    earlier = jnp.where(chip == 0, 0.0, tail_in[...])
    previous = pltpu.roll(earlier, lax.rem(width, OVL), axis=1)
    for comp in range(2):
        head = img[pl.ds(32 * comp, ROWS, stride=64), :]
        before = previous[ROWS * comp : ROWS * comp + ROWS]
        mixed = jnp.where(inside, (1.0 - ramp) * before + ramp * head, head)
        img[pl.ds(32 * comp, ROWS, stride=64), :] = mixed
        mixed = mixed * mixed
        energy = energy + mixed[:8] + mixed[8:16] + mixed[16:]
    esend[...] = energy

    def share(k):
        return pltpu.make_async_remote_copy(
            src_ref=esend,
            dst_ref=erecv.at[k],
            send_sem=esend_sem.at[k],
            recv_sem=erecv_sem.at[k],
            device_id={"line": lax.rem(me + k, LINES)},
            device_id_type=MESH,
        )

    @pl.loop(1, LINES)
    def _(k):
        share(k).start()

    for c in range(2):

        @pl.loop(0, LINES)
        def _(k, c=c):
            onward(c, k).wait_send()

        @pl.loop(1, LINES)
        def _(k, c=c):
            direct(c, k).wait_send()

    erecv[0] = energy

    @pl.loop(1, LINES)
    def _(k):
        share(k).wait_recv()

    total = jnp.sum(jnp.sum(erecv[...], axis=0), axis=(0, 1), keepdims=True)
    scale = lax.rsqrt(total / (RKEEP * AZ) + 1e-06)

    @pl.loop(0, ROWS)
    def _(r):
        for comp in range(2):
            v = img[pl.ds(pl.multiple_of(64 * r + 32 * comp, 32), 32), :]
            out_ref[comp, r] = (v * scale).astype(BF16)

    @pl.loop(1, LINES)
    def _(k):
        share(k).wait_send()


def local(echoes, range_filter, rcmc_weights, fm_rate, rcmc_shift, seam_width, seam_link):
    import functools

    weights = rcmc_weights.reshape(TAPS, 128, 32).transpose(0, 2, 1)
    vmem = pl.BlockSpec(memory_space=pltpu.VMEM)
    smem = pl.BlockSpec(memory_space=pltpu.SMEM)
    hbm = pl.BlockSpec(memory_space=pl.ANY)
    dma = pltpu.SemaphoreType.DMA
    image = pl.pallas_call(
        functools.partial(kernel, lax.axis_size("chip")),
        out_shape=jax.ShapeDtypeStruct((2, ROWS, 32, 128), BF16),
        in_specs=[hbm, vmem, vmem, smem, smem, smem, smem] + [vmem] * 8,
        out_specs=vmem,
        scratch_shapes=[
            pltpu.VMEM((2, 256, 4096), BF16),
            pltpu.VMEM((64, 128), F32),
            pltpu.VMEM((80, 128), F32),
            pltpu.VMEM((4, 34 * 128, 128), BF16),
            pltpu.VMEM((RKEEP, 256), F32),
            pltpu.VMEM((2, 48 * LINES, 128), F32),
            pltpu.VMEM((2 * LINES * SLOT, 128), F32),
            pltpu.VMEM((32 * NEED, 256), BF16),
            pltpu.VMEM((32 * NEED, 256), BF16),
            pltpu.VMEM((NEED, 32, 256), F32),
            pltpu.VMEM((ROWS, 32, 128), F32),
            pltpu.VMEM((ROWS, 32, 128), F32),
            pltpu.VMEM((32 * ROWS, 256), BF16),
            pltpu.VMEM((32 * ROWS, 256), BF16),
            pltpu.VMEM((32 * ROWS, 256), F32),
            pltpu.VMEM((64 * ROWS, 128), F32),
            pltpu.VMEM((2 * ROWS, 128), F32),
            pltpu.VMEM((2 * ROWS, 128), F32),
            pltpu.VMEM((8, 128), F32),
            pltpu.VMEM((LINES, 8, 128), F32),
            dma((2,)),
            dma((2, LINES)),
            dma((2, LINES)),
            dma((2, LINES)),
            dma((2, LINES)),
            dma((2,)),
            dma((LINES,)),
            dma((LINES,)),
        ],
        compiler_params=pltpu.CompilerParams(
            collective_id=0, has_side_effects=True, vmem_limit_bytes=48 * 1024 * 1024
        ),
        name="focus",
    )(
        echoes,
        range_filter,
        weights,
        fm_rate,
        rcmc_shift,
        seam_width,
        seam_link,
        *(jnp.asarray(t) for t in tables()),
    )
    return image.reshape(1, 2, ROWS, AZ)


def solution(mesh):
    in_specs = (
        P("chip", None, "line", None),
        P(),
        P(),
        P("chip", "line"),
        P("chip", "line"),
        P("chip"),
        P("chip"),
    )
    out_specs = P("chip", None, "line", None)
    return jax.shard_map(local, mesh=mesh, in_specs=in_specs, out_specs=out_specs, check_vma=False)
```

```python
import math

import jax
import jax.numpy as jnp
import numpy as np
from jax import lax
from jax.experimental import pallas as pl
from jax.experimental.pallas import tpu as pltpu
from jax.sharding import PartitionSpec as P

F32 = jnp.float32
BF16 = jnp.bfloat16
AZ = 4096
RKEEP = 384
TAPS = 8
OVL = 128
LINES = 16
ROWS = RKEEP // LINES
NEED = 44
SLOT = 104
HIGHEST = lax.Precision.HIGHEST
MESH = pl.DeviceIdType.MESH


def place(comp, i):
    if i < 16:
        return comp * 16 + i
    if i < 20:
        return 32 + comp * 4 + i - 16
    return 40 + comp * 4 + i - 20


def split(value):
    high = value.astype(BF16)
    return high, (value - high.astype(F32)).astype(BF16)


def angles(rows, columns, length, sign):
    product = np.outer(np.asarray(rows, np.int64), np.asarray(columns, np.int64)) % length
    theta = sign * 2.0 * np.pi / length * product
    return np.cos(theta), np.sin(theta)


def split_table(table, axis):
    import ml_dtypes

    high = table.astype(np.float32).astype(ml_dtypes.bfloat16)
    low = (table - high.astype(np.float64)).astype(np.float32).astype(ml_dtypes.bfloat16)
    return np.concatenate([high, high, low], axis=axis)


def tables():
    n32, n128 = np.arange(32), np.arange(128)
    c, s = angles(n32, n32, 32, -1)
    first = np.block([[c, -s], [s, c]])
    filter_turn = np.stack(angles(n32, n128, 4096, -1))
    shift = (4 * n32[None, :] - np.arange(4)[:, None]).reshape(-1)
    c, s = angles(shift, n128, 128, 1)
    second = np.block([[c, -s], [s, c]]) / 4096.0
    c, s = angles(n32, n32, 32, -1)
    forward32 = np.block([[c, -s], [s, c]])
    turn = np.stack(angles(n32, n128, 4096, -1))
    c, s = angles(n128, n128, 128, -1)
    forward128 = np.block([[c, s], [-s, c]])
    c, s = angles(n128, n128, 128, 1)
    inverse128 = np.block([[c, s], [-s, c]])
    c, s = angles(n32, n32, 32, 1)
    inverse32 = np.block([[c, -s], [s, c]]) / 4096.0
    f32 = lambda t: t.astype(np.float32)
    return (
        f32(first),
        f32(filter_turn),
        f32(second),
        split_table(forward32, 1),
        f32(turn),
        split_table(forward128, 0),
        split_table(inverse128, 0),
        split_table(inverse32, 1),
    )


def mm(a, b, precision=None):
    return lax.dot_general(
        a, b, (((1,), (0,)), ((), ())), precision=precision, preferred_element_type=F32
    )


def mm_nt(a, b, precision=None):
    return lax.dot_general(
        a, b, (((1,), (1,)), ((), ())), precision=precision, preferred_element_type=F32
    )


def turned(real, imag, c, s):
    return real * c - imag * s, real * s + imag * c


def kernel(
    chips,
    echo_hbm,
    filter_hbm,
    weight_hbm,
    rate_hbm,
    shift_hbm,
    width_ref,
    link_ref,
    first_hbm,
    fturn_hbm,
    second_hbm,
    fwd32_hbm,
    turn_hbm,
    fwd128_hbm,
    inv128_hbm,
    inv32_hbm,
    out_ref,
    filter_ref,
    weight_ref,
    rate_ref,
    shift_ref,
    first_ref,
    fturn_ref,
    second_ref,
    fwd32_ref,
    turn_ref,
    fwd128_ref,
    inv128_ref,
    inv32_ref,
    echo,
    spectrum,
    pulse,
    band,
    acc,
    piece,
    recv,
    gathered,
    weights,
    mid_hi,
    mid_lo,
    ext,
    cosine,
    sine,
    foc_hi,
    foc_lo,
    back,
    img,
    tail,
    tail_in,
    esend,
    erecv,
    table_sem,
    load_sem,
    send_sem,
    recv_sem,
    hsend_sem,
    hrecv_sem,
    fsend_sem,
    tail_sem,
    esend_sem,
    erecv_sem,
):
    me = lax.axis_index("line")
    chip = lax.axis_index("chip")
    following = lax.rem(chip + 1, chips)
    preceding = lax.rem(chip + chips - 1, chips)
    barrier = pltpu.get_barrier_semaphore()

    @pl.loop(1, LINES)
    def _(k):
        pl.semaphore_signal(
            barrier, inc=1, device_id={"line": lax.rem(me + k, LINES)}, device_id_type=MESH
        )

    pl.semaphore_signal(barrier, inc=1, device_id={"chip": following}, device_id_type=MESH)
    pl.semaphore_signal(barrier, inc=1, device_id={"chip": preceding}, device_id_type=MESH)

    def load(c):
        return pltpu.make_async_copy(
            echo_hbm.at[0, :, pl.ds(128 * c, 128), :],
            echo.at[:, pl.ds(128 * c, 128), :],
            load_sem.at[c],
        )

    pairs = (
        (filter_hbm, filter_ref),
        (first_hbm, first_ref),
        (fturn_hbm, fturn_ref),
        (second_hbm, second_ref),
        (rate_hbm, rate_ref),
        (shift_hbm, shift_ref),
        (weight_hbm, weight_ref),
        (fwd32_hbm, fwd32_ref),
        (turn_hbm, turn_ref),
        (fwd128_hbm, fwd128_ref),
        (inv128_hbm, inv128_ref),
        (inv32_hbm, inv32_ref),
    )
    fetch = [
        pltpu.make_async_copy(a, b, table_sem.at[i]) for i, (a, b) in enumerate(pairs)
    ]
    for copy in fetch[:4]:
        copy.start()
    load(0).start()
    load(1).start()
    for copy in fetch[4:]:
        copy.start()
    for c in range(2):
        piece[c, pl.ds(48 * LINES, 40), :] = jnp.zeros((40, 128), F32)
    for copy in fetch[:4]:
        copy.wait()

    for comp in range(2):
        for a in range(32):
            spectrum[pl.ds(comp * 32 + a, 1), :] = filter_ref[comp : comp + 1, 128 * a : 128 * a + 128]
    y = mm(first_ref[...], spectrum[...], HIGHEST)
    yr, yi = turned(y[:32], y[32:], fturn_ref[0], fturn_ref[1])
    y = mm_nt(second_ref[...], jnp.concatenate([yr, yi], axis=1), HIGHEST)
    for comp in range(2):
        rows = jnp.concatenate(
            [y[128 * comp + 32 * u : 128 * comp + 32 * u + 32] for u in range(4)], axis=1
        )
        pulse[pl.ds(40 * comp, 32), :] = rows
        pulse[pl.ds(40 * comp + 32, 8), :] = rows[:8]

    keep = lax.broadcasted_iota(jnp.int32, (128, 128), 1) >= lax.broadcasted_iota(
        jnp.int32, (128, 128), 0
    )

    def slanted(comp, m):
        row = pulse[pl.ds(40 * comp + m, 1), :]
        return pltpu.roll(
            jnp.broadcast_to(row, (128, 128)), 0, axis=1, stride=1, stride_axis=0
        )

    def build(m, carry):
        new = []
        at = pl.multiple_of(128 * m, 128)
        for comp in range(2):
            ahead = slanted(comp, m + 1)
            high, low = split(jnp.where(keep, carry[comp], ahead))
            band[2 * comp, pl.ds(at, 128), :] = high
            band[2 * comp + 1, pl.ds(at, 128), :] = low
            new.append(ahead)
        return tuple(new)

    def step(c, t, at0, at1):
        s = pl.multiple_of(256 * t, 256)
        xr = echo[0, 128 * c : 128 * c + 128, pl.ds(s, 256)]
        xi = echo[1, 128 * c : 128 * c + 128, pl.ds(s, 256)]
        right = jnp.concatenate(
            [
                jnp.concatenate([xr, xr, -xi, -xi], axis=1),
                jnp.concatenate([xi, xi, xr, xr], axis=1),
            ],
            axis=0,
        )
        left = jnp.concatenate(
            [
                band[part, pl.ds(pl.multiple_of(128 * at, 128), RKEEP), :]
                for part in range(4)
                for at in (at0, at1)
            ],
            axis=1,
        )
        acc[...] += mm_nt(left, right)

    def pack(c):
        for g in range(LINES):
            ramp = lax.broadcasted_iota(jnp.int32, (ROWS, 1), 0) + ROWS * g
            gain = 1.0 + 2.0 * ramp.astype(F32) / RKEEP
            for comp in range(2):
                v = acc[ROWS * g : ROWS * g + ROWS, 128 * comp : 128 * comp + 128] * gain
                base = 48 * g
                piece[c, base + 16 * comp : base + 16 * comp + 16, :] = v[:16]
                piece[c, base + 32 + 4 * comp : base + 36 + 4 * comp, :] = v[16:20]
                piece[c, base + 40 + 4 * comp : base + 44 + 4 * comp, :] = v[20:]

    acc[...] = jnp.zeros_like(acc)
    carry = lax.fori_loop(0, 5, build, (slanted(0, 0), slanted(1, 0)))
    load(0).wait()

    def first_pass(i, carry):
        carry = build(2 * i + 6, build(2 * i + 5, carry))
        step(0, 15 - i, 2 * i + 2, 2 * i + 1)
        return carry

    lax.fori_loop(0, 15, first_pass, carry)
    step(0, 0, 0, 31)
    pack(0)

    odd = lax.rem(me, 2) == 1

    def order(j):
        return jnp.where(lax.rem(j, 2) == 0, 15 - j // 2, (j + 1) // 2)

    def slot_of(source, c):
        return (2 * source + c) * SLOT

    def direct(c, k):
        to = lax.rem(me + k, LINES)
        return pltpu.make_async_remote_copy(
            src_ref=piece.at[c, pl.ds(pl.multiple_of(48 * to, 8), 48), :],
            dst_ref=recv.at[pl.ds(pl.multiple_of(slot_of(me, c), 8), 48), :],
            send_sem=send_sem.at[c, k],
            recv_sem=recv_sem.at[c, k],
            device_id={"line": to},
            device_id_type=MESH,
        )

    def margin(c, k):
        to = lax.rem(me + k, LINES)
        return pltpu.make_async_remote_copy(
            src_ref=piece.at[c, pl.ds(pl.multiple_of(48 * to + 48, 8), 40), :],
            dst_ref=recv.at[pl.ds(pl.multiple_of(slot_of(me, c) + 48, 8), 40), :],
            send_sem=hsend_sem.at[c, k],
            recv_sem=hrecv_sem.at[c, k],
            device_id={"line": to},
            device_id_type=MESH,
        )

    def onward(c, k):
        slot = slot_of(lax.rem(me + LINES - k, LINES), c)
        return pltpu.make_async_remote_copy(
            src_ref=recv.at[pl.ds(pl.multiple_of(slot, 8), 40), :],
            dst_ref=recv.at[pl.ds(pl.multiple_of(slot + 48, 8), 40), :],
            send_sem=fsend_sem.at[c, k],
            recv_sem=hrecv_sem.at[c, k],
            device_id={"line": lax.rem(me + LINES - 1, LINES)},
            device_id_type=MESH,
        )

    def to_odd(k):
        return lax.rem(me + k, 2) == 1

    def send(c):
        @pl.loop(0, LINES - 1)
        def _(j):
            k = order(j)
            direct(c, k).start()

            @pl.when(to_odd(k))
            def _():
                margin(c, k).start()

        own = pl.multiple_of(48 * me, 8)
        at = pl.multiple_of(slot_of(me, c), 8)
        recv[pl.ds(at, 48), :] = piece[c, pl.ds(own, 48), :]

        @pl.when(odd)
        def _():
            recv[pl.ds(at + 48, 40), :] = piece[c, pl.ds(pl.multiple_of(own + 48, 8), 40), :]
            onward(c, 0).start()

    def hand_on(c):
        @pl.loop(0, LINES - 1)
        def _(j):
            k = order(j)
            direct(c, k).wait_recv()

            @pl.when(odd)
            def _():
                onward(c, k).start()

    pl.semaphore_wait(barrier, LINES + 1)
    send(0)
    acc[...] = jnp.zeros_like(acc)
    load(1).wait()

    @pl.loop(0, 16)
    def _(t):
        step(1, t, lax.rem(32 - 2 * t, 32), 31 - 2 * t)

    pack(1)
    send(1)
    for copy in fetch[4:]:
        copy.wait()
    hand_on(0)

    for a in range(32):
        gathered[8 * a : 8 * a + 8, :] = weight_ref[:, 128 * a : 128 * a + 128]
    row = lax.broadcasted_iota(jnp.int32, (128, 128), 0)
    target = 4 * lax.rem(row, 32) + row // 32
    spread = (lax.broadcasted_iota(jnp.int32, (128, 128), 1) == target).astype(F32).astype(BF16)
    spread = jnp.concatenate([spread, spread, spread], axis=0)
    for t in range(TAPS):
        v = gathered[pl.ds(t, 32, stride=8), :].T
        v = jnp.concatenate([v[32 * u : 32 * u + 32] for u in range(4)], axis=1)
        high = v.astype(BF16)
        middle, low = split(v - high.astype(F32))
        weights[t] = mm(jnp.concatenate([high, middle, low], axis=1), spread)

    index = lax.broadcasted_iota(jnp.int32, (32, 128), 0) + 32 * lax.broadcasted_iota(
        jnp.int32, (32, 128), 1
    )
    frequency = jnp.where(index < AZ // 2, index, index - AZ).astype(F32) / AZ
    squared = frequency * frequency

    @pl.loop(0, ROWS)
    def _(r):
        turns = rate_ref[0, r] * squared
        turns = turns - 2.0 * jnp.round(turns * 0.5)
        cosine[r] = jnp.cos(math.pi * turns)
        sine[r] = jnp.sin(math.pi * turns)

    hand_on(1)

    tc, ts = turn_ref[0], turn_ref[1]

    def column(i):
        def part(comp):
            at = place(comp, i) if i < ROWS else 48 + place(comp, i - ROWS)
            return recv[pl.ds(at, 32, stride=SLOT), :]

        return jnp.concatenate([part(0), part(1)], axis=0)

    def across(first, last):
        for i in range(first, last, 2):
            high, low = split(jnp.concatenate([column(i), column(i + 1)], axis=1))
            y = mm(fwd32_ref[...], jnp.concatenate([high, low, high], axis=0))
            for j in range(2):
                yr, yi = turned(
                    y[:32, 128 * j : 128 * j + 128], y[32:, 128 * j : 128 * j + 128], tc, ts
                )
                high_j, low_j = split(jnp.concatenate([yr, yi], axis=1))
                mid_hi[32 * (i + j) : 32 * (i + j) + 32, :] = high_j
                mid_lo[32 * (i + j) : 32 * (i + j) + 32, :] = low_j

    across(0, ROWS)
    for c in range(2):

        @pl.loop(0, LINES - 1)
        def _(j, c=c):
            margin(c, order(j)).wait_recv()

        @pl.when(jnp.logical_not(odd))
        def _(c=c):
            margin(c, 0).wait_recv()

    across(ROWS, NEED)

    @pl.loop(0, 4)
    def _(j):
        at = pl.multiple_of(352 * j, 32)
        high, low = mid_hi[pl.ds(at, 352), :], mid_lo[pl.ds(at, 352), :]
        y = mm(jnp.concatenate([high, low, high], axis=1), fwd128_ref[...])
        ext[pl.ds(11 * j, 11)] = y.reshape(11, 32, 256)

    @pl.loop(0, ROWS)
    def _(r):
        at = r + shift_ref[0, r]
        real = jnp.zeros((32, 128), F32)
        imag = jnp.zeros((32, 128), F32)
        for t in range(TAPS):
            w = weights[t]
            row = ext[at + t]
            real += w * row[:, :128]
            imag += w * row[:, 128:]
        fr, fi = turned(real, imag, cosine[r], -sine[r])
        high, low = split(jnp.concatenate([fr, fi], axis=1))
        foc_hi[pl.ds(pl.multiple_of(32 * r, 32), 32), :] = high
        foc_lo[pl.ds(pl.multiple_of(32 * r, 32), 32), :] = low

    @pl.loop(0, 3)
    def _(j):
        at = pl.multiple_of(256 * j, 256)
        high, low = foc_hi[pl.ds(at, 256), :], foc_lo[pl.ds(at, 256), :]
        back[pl.ds(at, 256), :] = mm(jnp.concatenate([high, low, high], axis=1), inv128_ref[...])

    for i in range(0, ROWS, 2):
        both = []
        for j in range(2):
            v = back[32 * (i + j) : 32 * (i + j) + 32, :]
            vr, vi = turned(v[:, :128], v[:, 128:], tc, -ts)
            both.append(jnp.concatenate([vr, vi], axis=0))
        high, low = split(jnp.concatenate(both, axis=1))
        y = mm(inv32_ref[...], jnp.concatenate([high, low, high], axis=0))
        for j in range(2):
            img[64 * (i + j) : 64 * (i + j) + 64, :] = y[:, 128 * j : 128 * j + 128]

    for comp in range(2):
        tail[ROWS * comp : ROWS * comp + ROWS, :] = img[pl.ds(32 * comp + 31, ROWS, stride=64), :]
    handed = pltpu.make_async_remote_copy(
        src_ref=tail,
        dst_ref=tail_in,
        send_sem=tail_sem.at[0],
        recv_sem=tail_sem.at[1],
        device_id={"chip": following},
        device_id_type=MESH,
    )
    handed.start()

    rest = (lax.broadcasted_iota(jnp.int32, (8, 128), 0) > 0).astype(F32)

    def gather(r, total):
        v = img[pl.ds(pl.multiple_of(64 * r, 64), 64), :]
        v = v * v
        for j in range(8):
            part = v[8 * j : 8 * j + 8]
            total = total + (part * rest if j % 4 == 0 else part)
        return total

    energy = lax.fori_loop(0, ROWS, gather, jnp.zeros((8, 128), F32))

    handed.wait()
    width = width_ref[0]
    lane = lax.broadcasted_iota(jnp.int32, (1, 128), 1)
    ramp = (lane.astype(F32) + 0.5) / width.astype(F32)
    linked = (link_ref[0] == 1).astype(jnp.int32)
    inside = lane < width * linked
    earlier = jnp.where(chip == 0, 0.0, tail_in[...])
    previous = pltpu.roll(earlier, lax.rem(width, OVL), axis=1)
    for comp in range(2):
        head = img[pl.ds(32 * comp, ROWS, stride=64), :]
        before = previous[ROWS * comp : ROWS * comp + ROWS]
        mixed = jnp.where(inside, (1.0 - ramp) * before + ramp * head, head)
        img[pl.ds(32 * comp, ROWS, stride=64), :] = mixed
        mixed = mixed * mixed
        energy = energy + mixed[:8] + mixed[8:16] + mixed[16:]
    esend[...] = energy

    def share(k):
        return pltpu.make_async_remote_copy(
            src_ref=esend,
            dst_ref=erecv.at[k],
            send_sem=esend_sem.at[k],
            recv_sem=erecv_sem.at[k],
            device_id={"line": lax.rem(me + k, LINES)},
            device_id_type=MESH,
        )

    @pl.loop(1, LINES)
    def _(k):
        share(k).start()

    for c in range(2):

        @pl.loop(1, LINES)
        def _(k, c=c):
            direct(c, k).wait_send()

            @pl.when(to_odd(k))
            def _():
                margin(c, k).wait_send()

        @pl.when(odd)
        def _(c=c):
            @pl.loop(0, LINES)
            def _(k):
                onward(c, k).wait_send()

    erecv[0] = energy

    @pl.loop(1, LINES)
    def _(k):
        share(k).wait_recv()

    total = jnp.sum(jnp.sum(erecv[...], axis=0), axis=(0, 1), keepdims=True)
    scale = lax.rsqrt(total / (RKEEP * AZ) + 1e-06)

    @pl.loop(0, ROWS)
    def _(r):
        for comp in range(2):
            v = img[pl.ds(pl.multiple_of(64 * r + 32 * comp, 32), 32), :]
            out_ref[comp, r] = (v * scale).astype(BF16)

    @pl.loop(1, LINES)
    def _(k):
        share(k).wait_send()


def local(echoes, range_filter, rcmc_weights, fm_rate, rcmc_shift, seam_width, seam_link):
    import functools

    vmem = pl.BlockSpec(memory_space=pltpu.VMEM)
    smem = pl.BlockSpec(memory_space=pltpu.SMEM)
    hbm = pl.BlockSpec(memory_space=pltpu.HBM)
    dma = pltpu.SemaphoreType.DMA
    image = pl.pallas_call(
        functools.partial(kernel, lax.axis_size("chip")),
        out_shape=jax.ShapeDtypeStruct((2, ROWS, 32, 128), BF16),
        in_specs=[hbm] * 5 + [smem] * 2 + [hbm] * 8,
        out_specs=vmem,
        scratch_shapes=[
            pltpu.VMEM((2, 4096), F32),
            pltpu.VMEM((TAPS, 4096), F32),
            pltpu.SMEM((1, ROWS), F32),
            pltpu.SMEM((1, ROWS), jnp.int32),
            pltpu.VMEM((64, 64), F32),
            pltpu.VMEM((2, 32, 128), F32),
            pltpu.VMEM((256, 256), F32),
            pltpu.VMEM((64, 192), BF16),
            pltpu.VMEM((2, 32, 128), F32),
            pltpu.VMEM((768, 256), BF16),
            pltpu.VMEM((768, 256), BF16),
            pltpu.VMEM((64, 192), BF16),
            pltpu.VMEM((2, 256, 4096), BF16),
            pltpu.VMEM((64, 128), F32),
            pltpu.VMEM((80, 128), F32),
            pltpu.VMEM((4, 35 * 128, 128), BF16),
            pltpu.VMEM((RKEEP, 256), F32),
            pltpu.VMEM((2, 48 * LINES + 40, 128), F32),
            pltpu.VMEM((2 * LINES * SLOT, 128), F32),
            pltpu.VMEM((32 * TAPS, 128), F32),
            pltpu.VMEM((TAPS, 32, 128), F32),
            pltpu.VMEM((32 * NEED, 256), BF16),
            pltpu.VMEM((32 * NEED, 256), BF16),
            pltpu.VMEM((NEED, 32, 256), F32),
            pltpu.VMEM((ROWS, 32, 128), F32),
            pltpu.VMEM((ROWS, 32, 128), F32),
            pltpu.VMEM((32 * ROWS, 256), BF16),
            pltpu.VMEM((32 * ROWS, 256), BF16),
            pltpu.VMEM((32 * ROWS, 256), F32),
            pltpu.VMEM((64 * ROWS, 128), F32),
            pltpu.VMEM((2 * ROWS, 128), F32),
            pltpu.VMEM((2 * ROWS, 128), F32),
            pltpu.VMEM((8, 128), F32),
            pltpu.VMEM((LINES, 8, 128), F32),
            dma((12,)),
            dma((2,)),
            dma((2, LINES)),
            dma((2, LINES)),
            dma((2, LINES)),
            dma((2, LINES)),
            dma((2, LINES)),
            dma((2,)),
            dma((LINES,)),
            dma((LINES,)),
        ],
        compiler_params=pltpu.CompilerParams(
            collective_id=0, has_side_effects=True, vmem_limit_bytes=67_043_328
        ),
        name="focus",
    )(
        echoes,
        range_filter,
        rcmc_weights,
        fm_rate,
        rcmc_shift,
        seam_width,
        seam_link,
        *(jnp.asarray(t) for t in tables()),
    )
    return image.reshape(1, 2, ROWS, AZ)


def solution(mesh):
    in_specs = (
        P("chip", None, "line", None),
        P(),
        P(),
        P("chip", "line"),
        P("chip", "line"),
        P("chip"),
        P("chip"),
    )
    out_specs = P("chip", None, "line", None)
    return jax.shard_map(local, mesh=mesh, in_specs=in_specs, out_specs=out_specs, check_vma=False)
```

```python
import math

import jax
import jax.numpy as jnp
import numpy as np
from jax import lax
from jax.experimental import pallas as pl
from jax.experimental.pallas import tpu as pltpu
from jax.sharding import PartitionSpec as P

F32 = jnp.float32
BF16 = jnp.bfloat16
AZ = 4096
RKEEP = 384
TAPS = 8
OVL = 128
LINES = 16
ROWS = RKEEP // LINES
NEED = 44
PITCH = 72
SLOT = 104
HIGHEST = lax.Precision.HIGHEST
MESH = pl.DeviceIdType.MESH


def place(comp, i):
    if i < 16:
        return comp * 16 + i
    if i < 20:
        return 32 + comp * 4 + i - 16
    return 40 + comp * 4 + i - 20


def split(value):
    high = value.astype(BF16)
    return high, (value - high.astype(F32)).astype(BF16)


def angles(rows, columns, length, sign):
    product = np.outer(np.asarray(rows, np.int64), np.asarray(columns, np.int64)) % length
    theta = sign * 2.0 * np.pi / length * product
    return np.cos(theta), np.sin(theta)


def split_table(table, axis):
    import ml_dtypes

    high = table.astype(np.float32).astype(ml_dtypes.bfloat16)
    low = (table - high.astype(np.float64)).astype(np.float32).astype(ml_dtypes.bfloat16)
    return np.concatenate([high, high, low], axis=axis)


def tables():
    n32, n128 = np.arange(32), np.arange(128)
    c, s = angles(n32, n32, 32, -1)
    first = np.block([[c, -s], [s, c]])
    filter_turn = np.stack(angles(n32, n128, 4096, -1))
    shift = (4 * n32[None, :] - np.arange(4)[:, None]).reshape(-1)
    c, s = angles(shift, n128, 128, 1)
    second = np.block([[c, -s], [s, c]]) / 4096.0
    c, s = angles(n32, n32, 32, -1)
    forward32 = np.block([[c, -s], [s, c]])
    turn = np.stack(angles(n32, n128, 4096, -1))
    c, s = angles(n128, n128, 128, -1)
    forward128 = np.block([[c, s], [-s, c]])
    c, s = angles(n128, n128, 128, 1)
    inverse128 = np.block([[c, s], [-s, c]])
    c, s = angles(n32, n32, 32, 1)
    inverse32 = np.block([[c, -s], [s, c]]) / 4096.0
    ends = np.concatenate([inverse32[31::32], np.zeros((14, 64))])
    inverse32 = np.concatenate([inverse32, ends])
    f32 = lambda t: t.astype(np.float32)
    return (
        f32(first),
        f32(filter_turn),
        f32(second),
        split_table(forward32, 1),
        f32(turn),
        split_table(forward128, 0),
        split_table(inverse128, 0),
        split_table(inverse32, 1),
    )


def mm(a, b, precision=None):
    return lax.dot_general(
        a, b, (((1,), (0,)), ((), ())), precision=precision, preferred_element_type=F32
    )


def mm_nt(a, b, precision=None):
    return lax.dot_general(
        a, b, (((1,), (1,)), ((), ())), precision=precision, preferred_element_type=F32
    )


def turned(real, imag, c, s):
    return real * c - imag * s, real * s + imag * c


def kernel(
    chips,
    echo_hbm,
    filter_hbm,
    weight_hbm,
    rate_hbm,
    shift_hbm,
    width_ref,
    link_ref,
    first_hbm,
    fturn_hbm,
    second_hbm,
    fwd32_hbm,
    turn_hbm,
    fwd128_hbm,
    inv128_hbm,
    inv32_hbm,
    out_ref,
    filter_ref,
    weight_ref,
    rate_ref,
    shift_ref,
    first_ref,
    fturn_ref,
    second_ref,
    fwd32_ref,
    turn_ref,
    fwd128_ref,
    inv128_ref,
    inv32_ref,
    echo,
    spectrum,
    pulse,
    band,
    acc,
    piece,
    recv,
    gathered,
    weights,
    mid_hi,
    mid_lo,
    ext,
    cosine,
    sine,
    foc_hi,
    foc_lo,
    back,
    img,
    tail,
    tail_in,
    esend,
    erecv,
    table_sem,
    load_sem,
    send_sem,
    recv_sem,
    hsend_sem,
    hrecv_sem,
    fsend_sem,
    tail_sem,
    esend_sem,
    erecv_sem,
):
    me = lax.axis_index("line")
    chip = lax.axis_index("chip")
    following = lax.rem(chip + 1, chips)
    preceding = lax.rem(chip + chips - 1, chips)
    barrier = pltpu.get_barrier_semaphore()

    @pl.loop(1, LINES)
    def _(k):
        pl.semaphore_signal(
            barrier, inc=1, device_id={"line": lax.rem(me + k, LINES)}, device_id_type=MESH
        )

    pl.semaphore_signal(barrier, inc=1, device_id={"chip": following}, device_id_type=MESH)
    pl.semaphore_signal(barrier, inc=1, device_id={"chip": preceding}, device_id_type=MESH)

    def load(c):
        return pltpu.make_async_copy(
            echo_hbm.at[0, :, pl.ds(128 * c, 128), :],
            echo.at[:, pl.ds(128 * c, 128), :],
            load_sem.at[c],
        )

    pairs = (
        (filter_hbm, filter_ref),
        (first_hbm, first_ref),
        (fturn_hbm, fturn_ref),
        (second_hbm, second_ref),
        (rate_hbm, rate_ref),
        (shift_hbm, shift_ref),
        (weight_hbm, weight_ref),
        (fwd32_hbm, fwd32_ref),
        (turn_hbm, turn_ref),
        (fwd128_hbm, fwd128_ref),
        (inv128_hbm, inv128_ref),
        (inv32_hbm, inv32_ref),
    )
    fetch = [
        pltpu.make_async_copy(a, b, table_sem.at[i]) for i, (a, b) in enumerate(pairs)
    ]
    for copy in fetch[:4]:
        copy.start()
    load(0).start()
    load(1).start()
    for copy in fetch[4:]:
        copy.start()
    for c in range(2):
        piece[c, pl.ds(48 * LINES, 40), :] = jnp.zeros((40, 128), F32)
    for copy in fetch[:4]:
        copy.wait()

    for comp in range(2):
        for a in range(32):
            spectrum[pl.ds(comp * 32 + a, 1), :] = filter_ref[comp : comp + 1, 128 * a : 128 * a + 128]
    y = mm(first_ref[...], spectrum[...], HIGHEST)
    yr, yi = turned(y[:32], y[32:], fturn_ref[0], fturn_ref[1])
    y = mm_nt(second_ref[...], jnp.concatenate([yr, yi], axis=1), HIGHEST)
    for comp in range(2):
        rows = jnp.concatenate(
            [y[128 * comp + 32 * u : 128 * comp + 32 * u + 32] for u in range(4)], axis=1
        )
        pulse[pl.ds(40 * comp, 32), :] = rows
        pulse[pl.ds(40 * comp + 32, 8), :] = rows[:8]

    keep = lax.broadcasted_iota(jnp.int32, (128, 128), 1) >= lax.broadcasted_iota(
        jnp.int32, (128, 128), 0
    )

    def slanted(comp, m):
        row = pulse[pl.ds(40 * comp + m, 1), :]
        return pltpu.roll(
            jnp.broadcast_to(row, (128, 128)), 0, axis=1, stride=1, stride_axis=0
        )

    def build(m, carry):
        new = []
        at = pl.multiple_of(128 * m, 128)
        for comp in range(2):
            ahead = slanted(comp, m + 1)
            high, low = split(jnp.where(keep, carry[comp], ahead))
            band[2 * comp, pl.ds(at, 128), :] = high
            band[2 * comp + 1, pl.ds(at, 128), :] = low
            new.append(ahead)
        return tuple(new)

    def window(part, at, half):
        at = 128 * at
        if half is None:
            return band[part, pl.ds(pl.multiple_of(at, 128), RKEEP), :]
        return jnp.concatenate(
            [
                band[part, pl.ds(pl.multiple_of(at + 96 * j + 48 * half, 16), 48), :]
                for j in range(4)
            ],
            axis=0,
        )

    def step(c, t, at0, at1, half=None):
        s = pl.multiple_of(256 * t, 256)
        xr = echo[0, 128 * c : 128 * c + 128, pl.ds(s, 256)]
        xi = echo[1, 128 * c : 128 * c + 128, pl.ds(s, 256)]
        right = jnp.concatenate(
            [
                jnp.concatenate([xr, xr, -xi, -xi], axis=1),
                jnp.concatenate([xi, xi, xr, xr], axis=1),
            ],
            axis=0,
        )
        left = jnp.concatenate(
            [window(part, at, half) for part in range(4) for at in (at0, at1)], axis=1
        )
        acc[: left.shape[0], :] += mm_nt(left, right)

    def pack(c, half=None):
        for g in range(LINES):
            if half is not None and g // 2 % 2 != half:
                continue
            row = ROWS * g if half is None else 48 * (g // 4) + ROWS * (g % 2)
            ramp = lax.broadcasted_iota(jnp.int32, (ROWS, 1), 0) + ROWS * g
            gain = 1.0 + 2.0 * ramp.astype(F32) / RKEEP
            for comp in range(2):
                v = acc[row : row + ROWS, 128 * comp : 128 * comp + 128] * gain
                base = 48 * g
                piece[c, base + 16 * comp : base + 16 * comp + 16, :] = v[:16]
                piece[c, base + 32 + 4 * comp : base + 36 + 4 * comp, :] = v[16:20]
                piece[c, base + 40 + 4 * comp : base + 44 + 4 * comp, :] = v[20:]

    def clear():
        acc[...] = jnp.zeros_like(acc)

    def sweep(c, half=None):
        clear()

        @pl.loop(0, 16)
        def _(t):
            step(c, t, lax.rem(32 - 2 * t, 32), 31 - 2 * t, half)

        pack(c, half)

    clear()
    carry = (slanted(0, 0), slanted(1, 0))
    for m in range(5):
        carry = build(m, carry)
    load(0).wait()

    def first_pass(i, carry):
        carry = build(2 * i + 6, build(2 * i + 5, carry))
        step(0, 15 - i, 2 * i + 2, 2 * i + 1)
        return carry

    lax.fori_loop(0, 15, first_pass, carry)
    step(0, 0, 0, 31)
    pack(0)

    odd = lax.rem(me, 2) == 1

    def order(j):
        return jnp.where(lax.rem(j, 2) == 0, 15 - j // 2, (j + 1) // 2)

    def slot_of(source, c):
        return (2 * source + c) * SLOT

    def direct(c, k):
        to = lax.rem(me + k, LINES)
        return pltpu.make_async_remote_copy(
            src_ref=piece.at[c, pl.ds(pl.multiple_of(48 * to, 8), 48), :],
            dst_ref=recv.at[pl.ds(pl.multiple_of(slot_of(me, c), 8), 48), :],
            send_sem=send_sem.at[c, k],
            recv_sem=recv_sem.at[c, k],
            device_id={"line": to},
            device_id_type=MESH,
        )

    def margin(c, k):
        to = lax.rem(me + k, LINES)
        return pltpu.make_async_remote_copy(
            src_ref=piece.at[c, pl.ds(pl.multiple_of(48 * to + 48, 8), 40), :],
            dst_ref=recv.at[pl.ds(pl.multiple_of(slot_of(me, c) + 48, 8), 40), :],
            send_sem=hsend_sem.at[c, k],
            recv_sem=hrecv_sem.at[c, k],
            device_id={"line": to},
            device_id_type=MESH,
        )

    def onward(c, k):
        slot = slot_of(lax.rem(me + LINES - k, LINES), c)
        return pltpu.make_async_remote_copy(
            src_ref=recv.at[pl.ds(pl.multiple_of(slot, 8), 40), :],
            dst_ref=recv.at[pl.ds(pl.multiple_of(slot + 48, 8), 40), :],
            send_sem=fsend_sem.at[c, k],
            recv_sem=hrecv_sem.at[c, k],
            device_id={"line": lax.rem(me + LINES - 1, LINES)},
            device_id_type=MESH,
        )

    def each(action):
        @pl.loop(0, LINES - 1)
        def _(j):
            k = order(j)
            action(k, lax.rem(me + k, LINES))

    def start_direct(c, k, to, half=None):
        if half is None:
            direct(c, k).start()
        else:
            pl.when(lax.rem(to // 2, 2) == half)(lambda: direct(c, k).start())

    def start_margin(c, k, to):
        pl.when(lax.rem(to, 2) == 1)(lambda: margin(c, k).start())

    def keep_own(c):
        own = pl.multiple_of(48 * me, 8)
        at = pl.multiple_of(slot_of(me, c), 8)
        recv[pl.ds(at, 48), :] = piece[c, pl.ds(own, 48), :]

        @pl.when(odd)
        def _():
            recv[pl.ds(at + 48, 40), :] = piece[c, pl.ds(pl.multiple_of(own + 48, 8), 40), :]
            onward(c, 0).start()

    def hand_on(c, k):
        direct(c, k).wait_recv()
        pl.when(odd)(lambda: onward(c, k).start())

    pl.semaphore_wait(barrier, LINES + 1)

    def second(k, to):
        start_direct(0, k, to)
        start_margin(0, k, to)

    each(second)
    keep_own(0)
    load(1).wait()
    sweep(1)
    for copy in fetch[4:]:
        copy.wait()

    def third(k, to):
        hand_on(0, k)
        start_direct(1, k, to)
        start_margin(1, k, to)

    each(third)
    keep_own(1)
    for a in range(32):
        gathered[8 * a : 8 * a + 8, :] = weight_ref[:, 128 * a : 128 * a + 128]
    row = lax.broadcasted_iota(jnp.int32, (128, 128), 0)
    target = 4 * lax.rem(row, 32) + row // 32
    spread = (lax.broadcasted_iota(jnp.int32, (128, 128), 1) == target).astype(F32).astype(BF16)
    spread = jnp.concatenate([spread, spread, spread], axis=0)
    for t in range(TAPS):
        v = gathered[pl.ds(t, 32, stride=8), :].T
        v = jnp.concatenate([v[32 * u : 32 * u + 32] for u in range(4)], axis=1)
        high = v.astype(BF16)
        middle, low = split(v - high.astype(F32))
        weights[t] = mm(jnp.concatenate([high, middle, low], axis=1), spread)

    index = lax.broadcasted_iota(jnp.int32, (32, 128), 0) + 32 * lax.broadcasted_iota(
        jnp.int32, (32, 128), 1
    )
    frequency = jnp.where(index < AZ // 2, index, index - AZ).astype(F32) / AZ
    squared = frequency * frequency

    @pl.loop(0, ROWS)
    def _(r):
        turns = rate_ref[0, r] * squared
        turns = turns - 2.0 * jnp.round(turns * 0.5)
        cosine[r] = jnp.cos(math.pi * turns)
        sine[r] = jnp.sin(math.pi * turns)

    each(lambda k, to: hand_on(1, k))

    tc, ts = turn_ref[0], turn_ref[1]

    def column(i):
        def part(comp):
            at = place(comp, i) if i < ROWS else 48 + place(comp, i - ROWS)
            return recv[pl.ds(at, 32, stride=SLOT), :]

        return jnp.concatenate([part(0), part(1)], axis=0)

    def across(first, last):
        for i in range(first, last, 2):
            high, low = split(jnp.concatenate([column(i), column(i + 1)], axis=1))
            y = mm(fwd32_ref[...], jnp.concatenate([high, low, high], axis=0))
            for j in range(2):
                yr, yi = turned(
                    y[:32, 128 * j : 128 * j + 128], y[32:, 128 * j : 128 * j + 128], tc, ts
                )
                high_j, low_j = split(jnp.concatenate([yr, yi], axis=1))
                mid_hi[32 * (i + j) : 32 * (i + j) + 32, :] = high_j
                mid_lo[32 * (i + j) : 32 * (i + j) + 32, :] = low_j

    def along(first, count):
        @pl.loop(0, 2)
        def _(j):
            row = first + count // 2 * j
            at = pl.ds(pl.multiple_of(32 * row, 32), 16 * count)
            high, low = mid_hi[at, :], mid_lo[at, :]
            y = mm(jnp.concatenate([high, low, high], axis=1), fwd128_ref[...])
            ext[pl.ds(row, count // 2)] = y.reshape(count // 2, 32, 256)

    across(0, ROWS)
    along(0, ROWS)
    for c in range(2):

        @pl.loop(0, LINES - 1)
        def _(j, c=c):
            margin(c, order(j)).wait_recv()

        @pl.when(jnp.logical_not(odd))
        def _(c=c):
            margin(c, 0).wait_recv()

    across(ROWS, NEED)
    along(ROWS, NEED - ROWS)

    @pl.loop(0, ROWS, unroll=2)
    def _(r):
        at = r + shift_ref[0, r]
        real = jnp.zeros((32, 128), F32)
        imag = jnp.zeros((32, 128), F32)
        for t in range(TAPS):
            w = weights[t]
            row = ext[at + t]
            real += w * row[:, :128]
            imag += w * row[:, 128:]
        fr, fi = turned(real, imag, cosine[r], -sine[r])
        high, low = split(jnp.concatenate([fr, fi], axis=1))
        foc_hi[pl.ds(pl.multiple_of(32 * r, 32), 32), :] = high
        foc_lo[pl.ds(pl.multiple_of(32 * r, 32), 32), :] = low

    @pl.loop(0, 3)
    def _(j):
        at = pl.multiple_of(256 * j, 256)
        high, low = foc_hi[pl.ds(at, 256), :], foc_lo[pl.ds(at, 256), :]
        back[pl.ds(at, 256), :] = mm(jnp.concatenate([high, low, high], axis=1), inv128_ref[...])

    for i in range(0, ROWS, 2):
        both = []
        for j in range(2):
            v = back[32 * (i + j) : 32 * (i + j) + 32, :]
            vr, vi = turned(v[:, :128], v[:, 128:], tc, -ts)
            both.append(jnp.concatenate([vr, vi], axis=0))
        high, low = split(jnp.concatenate(both, axis=1))
        foc_hi[32 * i : 32 * i + 64, :] = high
        foc_lo[32 * i : 32 * i + 64, :] = low
        y = mm(inv32_ref[64:80, :], jnp.concatenate([high, low, high], axis=0))
        for j in range(2):
            for comp in range(2):
                row = ROWS * comp + i + j
                tail[row : row + 1, :] = y[comp : comp + 1, 128 * j : 128 * j + 128]

    handed = pltpu.make_async_remote_copy(
        src_ref=tail,
        dst_ref=tail_in,
        send_sem=tail_sem.at[0],
        recv_sem=tail_sem.at[1],
        device_id={"chip": following},
        device_id_type=MESH,
    )
    handed.start()

    for i in range(0, ROWS, 2):
        high, low = foc_hi[32 * i : 32 * i + 64, :], foc_lo[32 * i : 32 * i + 64, :]
        y = mm(inv32_ref[:64, :], jnp.concatenate([high, low, high], axis=0))
        for j in range(2):
            img[PITCH * (i + j) : PITCH * (i + j) + 64, :] = y[:, 128 * j : 128 * j + 128]

    rest = (lax.broadcasted_iota(jnp.int32, (8, 128), 0) > 0).astype(F32)

    def gather(r, total):
        v = img[pl.ds(pl.multiple_of(PITCH * r, 8), 64), :]
        v = v * v
        for j in range(8):
            part = v[8 * j : 8 * j + 8]
            total = total + (part * rest if j % 4 == 0 else part)
        return total

    energy = lax.fori_loop(0, ROWS, gather, jnp.zeros((8, 128), F32))

    handed.wait()
    width = width_ref[0]
    lane = lax.broadcasted_iota(jnp.int32, (1, 128), 1)
    ramp = (lane.astype(F32) + 0.5) / width.astype(F32)
    linked = (link_ref[0] == 1).astype(jnp.int32)
    inside = lane < width * linked
    earlier = jnp.where(chip == 0, 0.0, tail_in[...])
    previous = pltpu.roll(earlier, lax.rem(width, OVL), axis=1)
    for comp in range(2):
        head = img[pl.ds(32 * comp, ROWS, stride=PITCH), :]
        before = previous[ROWS * comp : ROWS * comp + ROWS]
        mixed = jnp.where(inside, (1.0 - ramp) * before + ramp * head, head)
        img[pl.ds(32 * comp, ROWS, stride=PITCH), :] = mixed
        mixed = mixed * mixed
        energy = energy + mixed[:8] + mixed[8:16] + mixed[16:]
    esend[...] = energy

    def share(k):
        return pltpu.make_async_remote_copy(
            src_ref=esend,
            dst_ref=erecv.at[k],
            send_sem=esend_sem.at[k],
            recv_sem=erecv_sem.at[k],
            device_id={"line": lax.rem(me + k, LINES)},
            device_id_type=MESH,
        )

    @pl.loop(1, LINES)
    def _(k):
        share(k).start()

    for c in range(2):

        @pl.loop(1, LINES)
        def _(k, c=c):
            direct(c, k).wait_send()

            @pl.when(lax.rem(me + k, 2) == 1)
            def _():
                margin(c, k).wait_send()

        @pl.when(odd)
        def _(c=c):
            @pl.loop(0, LINES)
            def _(k):
                onward(c, k).wait_send()

    erecv[0] = energy

    @pl.loop(1, LINES)
    def _(k):
        share(k).wait_recv()

    total = jnp.sum(jnp.sum(erecv[...], axis=0), axis=(0, 1), keepdims=True)
    scale = lax.rsqrt(total / (RKEEP * AZ) + 1e-06)

    @pl.loop(0, 32)
    def _(m):
        for comp in range(2):
            v = img[pl.ds(32 * comp + m, ROWS, stride=PITCH), :]
            at = pl.ds(pl.multiple_of(128 * m, 128), 128)
            out_ref[0, comp, :, at] = (v * scale).astype(BF16)

    @pl.loop(1, LINES)
    def _(k):
        share(k).wait_send()


def local(echoes, range_filter, rcmc_weights, fm_rate, rcmc_shift, seam_width, seam_link):
    import functools

    vmem = pl.BlockSpec(memory_space=pltpu.VMEM)
    smem = pl.BlockSpec(memory_space=pltpu.SMEM)
    hbm = pl.BlockSpec(memory_space=pltpu.HBM)
    dma = pltpu.SemaphoreType.DMA
    image = pl.pallas_call(
        functools.partial(kernel, lax.axis_size("chip")),
        out_shape=jax.ShapeDtypeStruct((1, 2, ROWS, AZ), BF16),
        in_specs=[hbm] * 5 + [smem] * 2 + [hbm] * 8,
        out_specs=vmem,
        scratch_shapes=[
            pltpu.VMEM((2, 4096), F32),
            pltpu.VMEM((TAPS, 4096), F32),
            pltpu.SMEM((1, ROWS), F32),
            pltpu.SMEM((1, ROWS), jnp.int32),
            pltpu.VMEM((64, 64), F32),
            pltpu.VMEM((2, 32, 128), F32),
            pltpu.VMEM((256, 256), F32),
            pltpu.VMEM((64, 192), BF16),
            pltpu.VMEM((2, 32, 128), F32),
            pltpu.VMEM((768, 256), BF16),
            pltpu.VMEM((768, 256), BF16),
            pltpu.VMEM((80, 192), BF16),
            pltpu.VMEM((2, 256, 4096), BF16),
            pltpu.VMEM((64, 128), F32),
            pltpu.VMEM((80, 128), F32),
            pltpu.VMEM((4, 35 * 128, 128), BF16),
            pltpu.VMEM((RKEEP, 256), F32),
            pltpu.VMEM((2, 48 * LINES + 40, 128), F32),
            pltpu.VMEM((2 * LINES * SLOT, 128), F32),
            pltpu.VMEM((32 * TAPS, 128), F32),
            pltpu.VMEM((TAPS, 32, 128), F32),
            pltpu.VMEM((32 * NEED, 256), BF16),
            pltpu.VMEM((32 * NEED, 256), BF16),
            pltpu.VMEM((NEED, 32, 256), F32),
            pltpu.VMEM((ROWS, 32, 128), F32),
            pltpu.VMEM((ROWS, 32, 128), F32),
            pltpu.VMEM((32 * ROWS, 256), BF16),
            pltpu.VMEM((32 * ROWS, 256), BF16),
            pltpu.VMEM((32 * ROWS, 256), F32),
            pltpu.VMEM((PITCH * ROWS, 128), F32),
            pltpu.VMEM((2 * ROWS, 128), F32),
            pltpu.VMEM((2 * ROWS, 128), F32),
            pltpu.VMEM((8, 128), F32),
            pltpu.VMEM((LINES, 8, 128), F32),
            dma((12,)),
            dma((2,)),
            dma((2, LINES)),
            dma((2, LINES)),
            dma((2, LINES)),
            dma((2, LINES)),
            dma((2, LINES)),
            dma((2,)),
            dma((LINES,)),
            dma((LINES,)),
        ],
        compiler_params=pltpu.CompilerParams(
            collective_id=0, has_side_effects=True, vmem_limit_bytes=67_043_328
        ),
        name="focus",
    )(
        echoes,
        range_filter,
        rcmc_weights,
        fm_rate,
        rcmc_shift,
        seam_width,
        seam_link,
        *(jnp.asarray(t) for t in tables()),
    )
    return image


def solution(mesh):
    in_specs = (
        P("chip", None, "line", None),
        P(),
        P(),
        P("chip", "line"),
        P("chip", "line"),
        P("chip"),
        P("chip"),
    )
    out_specs = P("chip", None, "line", None)
    return jax.shard_map(local, mesh=mesh, in_specs=in_specs, out_specs=out_specs, check_vma=False)
```

```python
import math

import jax
import jax.numpy as jnp
import numpy as np
from jax import lax
from jax.experimental import pallas as pl
from jax.experimental.pallas import tpu as pltpu
from jax.sharding import PartitionSpec as P

F32 = jnp.float32
BF16 = jnp.bfloat16
AZ = 4096
RKEEP = 384
TAPS = 8
OVL = 128
LINES = 16
ROWS = RKEEP // LINES
NEED = 44
PITCH = 72
SLOT = 104
HIGHEST = lax.Precision.HIGHEST
MESH = pl.DeviceIdType.MESH


def place(comp, i):
    if i < 16:
        return comp * 16 + i
    if i < 20:
        return 32 + comp * 4 + i - 16
    return 40 + comp * 4 + i - 20


def split(value):
    high = value.astype(BF16)
    return high, (value - high.astype(F32)).astype(BF16)


def angles(rows, columns, length, sign):
    product = np.outer(np.asarray(rows, np.int64), np.asarray(columns, np.int64)) % length
    theta = sign * 2.0 * np.pi / length * product
    return np.cos(theta), np.sin(theta)


def split_table(table, axis):
    import ml_dtypes

    high = table.astype(np.float32).astype(ml_dtypes.bfloat16)
    low = (table - high.astype(np.float64)).astype(np.float32).astype(ml_dtypes.bfloat16)
    return np.concatenate([high, high, low], axis=axis)


def tables():
    n32, n128 = np.arange(32), np.arange(128)
    c, s = angles(n32, n32, 32, -1)
    first = np.block([[c, -s], [s, c]])
    filter_turn = np.stack(angles(n32, n128, 4096, -1))
    shift = (4 * n32[None, :] - np.arange(4)[:, None]).reshape(-1)
    c, s = angles(shift, n128, 128, 1)
    second = np.block([[c, -s], [s, c]]) / 4096.0
    c, s = angles(n32, n32, 32, -1)
    forward32 = np.block([[c, -s], [s, c]])
    turn = np.stack(angles(n32, n128, 4096, -1))
    c, s = angles(n128, n128, 128, -1)
    forward128 = np.block([[c, s], [-s, c]])
    c, s = angles(n128, n128, 128, 1)
    inverse128 = np.block([[c, s], [-s, c]])
    c, s = angles(n32, n32, 32, 1)
    inverse32 = np.block([[c, -s], [s, c]]) / 4096.0
    ends = np.concatenate([inverse32[31::32], np.zeros((14, 64))])
    inverse32 = np.concatenate([inverse32, ends])
    f32 = lambda t: t.astype(np.float32)
    return (
        f32(first),
        f32(filter_turn),
        f32(second),
        split_table(forward32, 1),
        f32(turn),
        split_table(forward128, 0),
        split_table(inverse128, 0),
        split_table(inverse32, 1),
    )


def mm(a, b, precision=None):
    return lax.dot_general(
        a, b, (((1,), (0,)), ((), ())), precision=precision, preferred_element_type=F32
    )


def mm_nt(a, b, precision=None):
    return lax.dot_general(
        a, b, (((1,), (1,)), ((), ())), precision=precision, preferred_element_type=F32
    )


def turned(real, imag, c, s):
    return real * c - imag * s, real * s + imag * c


def kernel(
    chips,
    echo_hbm,
    filter_hbm,
    weight_hbm,
    rate_hbm,
    shift_hbm,
    width_ref,
    link_ref,
    first_hbm,
    fturn_hbm,
    second_hbm,
    fwd32_hbm,
    turn_hbm,
    fwd128_hbm,
    inv128_hbm,
    inv32_hbm,
    out_ref,
    filter_ref,
    weight_ref,
    rate_ref,
    shift_ref,
    first_ref,
    fturn_ref,
    second_ref,
    fwd32_ref,
    turn_ref,
    fwd128_ref,
    inv128_ref,
    inv32_ref,
    echo,
    spectrum,
    pulse,
    band,
    acc,
    piece,
    recv,
    gathered,
    weights,
    mid_hi,
    mid_lo,
    ext,
    cosine,
    sine,
    foc_hi,
    foc_lo,
    back,
    img,
    tail,
    tail_in,
    esend,
    erecv,
    table_sem,
    load_sem,
    send_sem,
    recv_sem,
    hsend_sem,
    hrecv_sem,
    fsend_sem,
    tail_sem,
    esend_sem,
    erecv_sem,
):
    me = lax.axis_index("line")
    chip = lax.axis_index("chip")
    following = lax.rem(chip + 1, chips)
    preceding = lax.rem(chip + chips - 1, chips)
    barrier = pltpu.get_barrier_semaphore()

    @pl.loop(1, LINES)
    def _(k):
        pl.semaphore_signal(
            barrier, inc=1, device_id={"line": lax.rem(me + k, LINES)}, device_id_type=MESH
        )

    pl.semaphore_signal(barrier, inc=1, device_id={"chip": following}, device_id_type=MESH)
    pl.semaphore_signal(barrier, inc=1, device_id={"chip": preceding}, device_id_type=MESH)

    def load(c):
        return pltpu.make_async_copy(
            echo_hbm.at[0, :, pl.ds(128 * c, 128), :],
            echo.at[:, pl.ds(128 * c, 128), :],
            load_sem.at[c],
        )

    pairs = (
        (filter_hbm, filter_ref),
        (first_hbm, first_ref),
        (fturn_hbm, fturn_ref),
        (second_hbm, second_ref),
        (rate_hbm, rate_ref),
        (shift_hbm, shift_ref),
        (weight_hbm, weight_ref),
        (fwd32_hbm, fwd32_ref),
        (turn_hbm, turn_ref),
        (fwd128_hbm, fwd128_ref),
        (inv128_hbm, inv128_ref),
        (inv32_hbm, inv32_ref),
    )
    fetch = [
        pltpu.make_async_copy(a, b, table_sem.at[i]) for i, (a, b) in enumerate(pairs)
    ]
    for copy in fetch[:4]:
        copy.start()
    load(0).start()
    load(1).start()
    for copy in fetch[4:]:
        copy.start()
    for c in range(2):
        piece[c, pl.ds(48 * LINES, 40), :] = jnp.zeros((40, 128), F32)
    for copy in fetch[:4]:
        copy.wait()

    for comp in range(2):
        for a in range(32):
            spectrum[pl.ds(comp * 32 + a, 1), :] = filter_ref[comp : comp + 1, 128 * a : 128 * a + 128]
    y = mm(first_ref[...], spectrum[...], HIGHEST)
    yr, yi = turned(y[:32], y[32:], fturn_ref[0], fturn_ref[1])
    y = mm_nt(second_ref[...], jnp.concatenate([yr, yi], axis=1), HIGHEST)
    for comp in range(2):
        rows = jnp.concatenate(
            [y[128 * comp + 32 * u : 128 * comp + 32 * u + 32] for u in range(4)], axis=1
        )
        pulse[pl.ds(40 * comp, 32), :] = rows
        pulse[pl.ds(40 * comp + 32, 8), :] = rows[:8]

    keep = lax.broadcasted_iota(jnp.int32, (128, 128), 1) >= lax.broadcasted_iota(
        jnp.int32, (128, 128), 0
    )

    def slanted(comp, m):
        row = pulse[pl.ds(40 * comp + m, 1), :]
        return pltpu.roll(
            jnp.broadcast_to(row, (128, 128)), 0, axis=1, stride=1, stride_axis=0
        )

    def build(m, carry):
        new = []
        at = pl.multiple_of(128 * m, 128)
        for comp in range(2):
            ahead = slanted(comp, m + 1)
            high, low = split(jnp.where(keep, carry[comp], ahead))
            band[2 * comp, pl.ds(at, 128), :] = high
            band[2 * comp + 1, pl.ds(at, 128), :] = low
            new.append(ahead)
        return tuple(new)

    def step(c, tiles):
        left, upper, lower = [], [], []
        for t, at0, at1 in tiles:
            s = pl.ds(pl.multiple_of(256 * t, 256), 256)
            xr = echo[0, 128 * c : 128 * c + 128, s]
            xi = echo[1, 128 * c : 128 * c + 128, s]
            upper += [xr, xr, -xi, -xi]
            lower += [xi, xi, xr, xr]
            left += [
                band[part, pl.ds(pl.multiple_of(128 * at, 128), RKEEP), :]
                for part in range(4)
                for at in (at0, at1)
            ]
        right = jnp.concatenate(
            [jnp.concatenate(upper, axis=1), jnp.concatenate(lower, axis=1)], axis=0
        )
        acc[...] += mm_nt(jnp.concatenate(left, axis=1), right)

    def pack(c):
        for g in range(LINES):
            row = ROWS * g
            ramp = lax.broadcasted_iota(jnp.int32, (ROWS, 1), 0) + ROWS * g
            gain = 1.0 + 2.0 * ramp.astype(F32) / RKEEP
            for comp in range(2):
                v = acc[row : row + ROWS, 128 * comp : 128 * comp + 128] * gain
                base = 48 * g
                piece[c, base + 16 * comp : base + 16 * comp + 16, :] = v[:16]
                piece[c, base + 32 + 4 * comp : base + 36 + 4 * comp, :] = v[16:20]
                piece[c, base + 40 + 4 * comp : base + 44 + 4 * comp, :] = v[20:]

    def clear():
        acc[...] = jnp.zeros_like(acc)

    def sweep(c):
        clear()

        @pl.loop(0, 8)
        def _(p):
            t = 2 * p
            step(
                c,
                [(t, lax.rem(32 - 2 * t, 32), 31 - 2 * t), (t + 1, 30 - 2 * t, 29 - 2 * t)],
            )

        pack(c)

    clear()
    carry = (slanted(0, 0), slanted(1, 0))
    for m in range(7):
        carry = build(m, carry)
    load(0).wait()

    def first_pass(p, carry):
        for m in range(4):
            carry = build(4 * p + 7 + m, carry)
        t = 15 - 2 * p
        step(0, [(t, 4 * p + 2, 4 * p + 1), (t - 1, 4 * p + 4, 4 * p + 3)])
        return carry

    lax.fori_loop(0, 7, first_pass, carry)
    step(0, [(1, 30, 29), (0, 0, 31)])
    pack(0)

    odd = lax.rem(me, 2) == 1

    def order(j):
        return jnp.where(lax.rem(j, 2) == 0, 15 - j // 2, (j + 1) // 2)

    def slot_of(source, c):
        return (2 * source + c) * SLOT

    def direct(c, k):
        to = lax.rem(me + k, LINES)
        return pltpu.make_async_remote_copy(
            src_ref=piece.at[c, pl.ds(pl.multiple_of(48 * to, 8), 48), :],
            dst_ref=recv.at[pl.ds(pl.multiple_of(slot_of(me, c), 8), 48), :],
            send_sem=send_sem.at[c, k],
            recv_sem=recv_sem.at[c, k],
            device_id={"line": to},
            device_id_type=MESH,
        )

    def margin(c, k):
        to = lax.rem(me + k, LINES)
        return pltpu.make_async_remote_copy(
            src_ref=piece.at[c, pl.ds(pl.multiple_of(48 * to + 48, 8), 40), :],
            dst_ref=recv.at[pl.ds(pl.multiple_of(slot_of(me, c) + 48, 8), 40), :],
            send_sem=hsend_sem.at[c, k],
            recv_sem=hrecv_sem.at[c, k],
            device_id={"line": to},
            device_id_type=MESH,
        )

    def onward(c, k):
        slot = slot_of(lax.rem(me + LINES - k, LINES), c)
        return pltpu.make_async_remote_copy(
            src_ref=recv.at[pl.ds(pl.multiple_of(slot, 8), 40), :],
            dst_ref=recv.at[pl.ds(pl.multiple_of(slot + 48, 8), 40), :],
            send_sem=fsend_sem.at[c, k],
            recv_sem=hrecv_sem.at[c, k],
            device_id={"line": lax.rem(me + LINES - 1, LINES)},
            device_id_type=MESH,
        )

    def each(action):
        @pl.loop(0, LINES - 1)
        def _(j):
            k = order(j)
            action(k, lax.rem(me + k, LINES))

    def start_margin(c, k, to):
        pl.when(lax.rem(to, 2) == 1)(lambda: margin(c, k).start())

    def keep_own(c):
        own = pl.multiple_of(48 * me, 8)
        at = pl.multiple_of(slot_of(me, c), 8)
        recv[pl.ds(at, 48), :] = piece[c, pl.ds(own, 48), :]

        @pl.when(odd)
        def _():
            recv[pl.ds(at + 48, 40), :] = piece[c, pl.ds(pl.multiple_of(own + 48, 8), 40), :]
            onward(c, 0).start()

    def hand_on(c, k):
        direct(c, k).wait_recv()
        pl.when(odd)(lambda: onward(c, k).start())

    pl.semaphore_wait(barrier, LINES + 1)

    def second(k, to):
        direct(0, k).start()
        start_margin(0, k, to)

    each(second)
    keep_own(0)
    load(1).wait()
    sweep(1)
    for copy in fetch[4:]:
        copy.wait()

    def third(k, to):
        hand_on(0, k)
        direct(1, k).start()
        start_margin(1, k, to)

    each(third)
    keep_own(1)
    for a in range(32):
        gathered[8 * a : 8 * a + 8, :] = weight_ref[:, 128 * a : 128 * a + 128]
    row = lax.broadcasted_iota(jnp.int32, (128, 128), 0)
    target = 4 * lax.rem(row, 32) + row // 32
    spread = (lax.broadcasted_iota(jnp.int32, (128, 128), 1) == target).astype(F32).astype(BF16)
    spread = jnp.concatenate([spread, spread, spread], axis=0)
    for t in range(TAPS):
        v = gathered[pl.ds(t, 32, stride=8), :].T
        v = jnp.concatenate([v[32 * u : 32 * u + 32] for u in range(4)], axis=1)
        high = v.astype(BF16)
        middle, low = split(v - high.astype(F32))
        weights[t] = mm(jnp.concatenate([high, middle, low], axis=1), spread)

    index = lax.broadcasted_iota(jnp.int32, (32, 128), 0) + 32 * lax.broadcasted_iota(
        jnp.int32, (32, 128), 1
    )
    frequency = jnp.where(index < AZ // 2, index, index - AZ).astype(F32) / AZ
    squared = frequency * frequency

    @pl.loop(0, ROWS)
    def _(r):
        turns = rate_ref[0, r] * squared
        turns = turns - 2.0 * jnp.round(turns * 0.5)
        cosine[r] = jnp.cos(math.pi * turns)
        sine[r] = jnp.sin(math.pi * turns)

    each(lambda k, to: hand_on(1, k))

    tc, ts = turn_ref[0], turn_ref[1]

    def column(i):
        def part(comp):
            at = place(comp, i) if i < ROWS else 48 + place(comp, i - ROWS)
            return recv[pl.ds(at, 32, stride=SLOT), :]

        return jnp.concatenate([part(0), part(1)], axis=0)

    def across(first, last):
        for i in range(first, last, 2):
            high, low = split(jnp.concatenate([column(i), column(i + 1)], axis=1))
            y = mm(fwd32_ref[...], jnp.concatenate([high, low, high], axis=0))
            for j in range(2):
                yr, yi = turned(
                    y[:32, 128 * j : 128 * j + 128], y[32:, 128 * j : 128 * j + 128], tc, ts
                )
                high_j, low_j = split(jnp.concatenate([yr, yi], axis=1))
                mid_hi[32 * (i + j) : 32 * (i + j) + 32, :] = high_j
                mid_lo[32 * (i + j) : 32 * (i + j) + 32, :] = low_j

    def along(first, count):
        @pl.loop(0, 2)
        def _(j):
            row = first + count // 2 * j
            at = pl.ds(pl.multiple_of(32 * row, 32), 16 * count)
            high, low = mid_hi[at, :], mid_lo[at, :]
            y = mm(jnp.concatenate([high, low, high], axis=1), fwd128_ref[...])
            ext[pl.ds(row, count // 2)] = y.reshape(count // 2, 32, 256)

    across(0, ROWS)
    along(0, ROWS)
    for c in range(2):

        @pl.loop(0, LINES - 1)
        def _(j, c=c):
            margin(c, order(j)).wait_recv()

        @pl.when(jnp.logical_not(odd))
        def _(c=c):
            margin(c, 0).wait_recv()

    across(ROWS, NEED)
    along(ROWS, NEED - ROWS)

    @pl.loop(0, ROWS, unroll=2)
    def _(r):
        at = r + shift_ref[0, r]
        real = jnp.zeros((32, 128), F32)
        imag = jnp.zeros((32, 128), F32)
        for t in range(TAPS):
            w = weights[t]
            row = ext[at + t]
            real += w * row[:, :128]
            imag += w * row[:, 128:]
        fr, fi = turned(real, imag, cosine[r], -sine[r])
        high, low = split(jnp.concatenate([fr, fi], axis=1))
        foc_hi[pl.ds(pl.multiple_of(32 * r, 32), 32), :] = high
        foc_lo[pl.ds(pl.multiple_of(32 * r, 32), 32), :] = low

    @pl.loop(0, 3)
    def _(j):
        at = pl.multiple_of(256 * j, 256)
        high, low = foc_hi[pl.ds(at, 256), :], foc_lo[pl.ds(at, 256), :]
        back[pl.ds(at, 256), :] = mm(jnp.concatenate([high, low, high], axis=1), inv128_ref[...])

    for i in range(0, ROWS, 2):
        both = []
        for j in range(2):
            v = back[32 * (i + j) : 32 * (i + j) + 32, :]
            vr, vi = turned(v[:, :128], v[:, 128:], tc, -ts)
            both.append(jnp.concatenate([vr, vi], axis=0))
        high, low = split(jnp.concatenate(both, axis=1))
        foc_hi[32 * i : 32 * i + 64, :] = high
        foc_lo[32 * i : 32 * i + 64, :] = low
        y = mm(inv32_ref[64:80, :], jnp.concatenate([high, low, high], axis=0))
        for j in range(2):
            for comp in range(2):
                row = ROWS * comp + i + j
                tail[row : row + 1, :] = y[comp : comp + 1, 128 * j : 128 * j + 128]

    handed = pltpu.make_async_remote_copy(
        src_ref=tail,
        dst_ref=tail_in,
        send_sem=tail_sem.at[0],
        recv_sem=tail_sem.at[1],
        device_id={"chip": following},
        device_id_type=MESH,
    )
    handed.start()

    for i in range(0, ROWS, 2):
        high, low = foc_hi[32 * i : 32 * i + 64, :], foc_lo[32 * i : 32 * i + 64, :]
        y = mm(inv32_ref[:64, :], jnp.concatenate([high, low, high], axis=0))
        for j in range(2):
            img[PITCH * (i + j) : PITCH * (i + j) + 64, :] = y[:, 128 * j : 128 * j + 128]

    rest = (lax.broadcasted_iota(jnp.int32, (8, 128), 0) > 0).astype(F32)

    def gather(r, total):
        v = img[pl.ds(pl.multiple_of(PITCH * r, 8), 64), :]
        v = v * v
        for j in range(8):
            part = v[8 * j : 8 * j + 8]
            total = total + (part * rest if j % 4 == 0 else part)
        return total

    energy = lax.fori_loop(0, ROWS, gather, jnp.zeros((8, 128), F32))

    handed.wait()
    width = width_ref[0]
    lane = lax.broadcasted_iota(jnp.int32, (1, 128), 1)
    ramp = (lane.astype(F32) + 0.5) / width.astype(F32)
    linked = (link_ref[0] == 1).astype(jnp.int32)
    inside = lane < width * linked
    earlier = jnp.where(chip == 0, 0.0, tail_in[...])
    previous = pltpu.roll(earlier, lax.rem(width, OVL), axis=1)
    for comp in range(2):
        head = img[pl.ds(32 * comp, ROWS, stride=PITCH), :]
        before = previous[ROWS * comp : ROWS * comp + ROWS]
        mixed = jnp.where(inside, (1.0 - ramp) * before + ramp * head, head)
        img[pl.ds(32 * comp, ROWS, stride=PITCH), :] = mixed
        mixed = mixed * mixed
        energy = energy + mixed[:8] + mixed[8:16] + mixed[16:]
    esend[...] = energy

    def share(k):
        return pltpu.make_async_remote_copy(
            src_ref=esend,
            dst_ref=erecv.at[k],
            send_sem=esend_sem.at[k],
            recv_sem=erecv_sem.at[k],
            device_id={"line": lax.rem(me + k, LINES)},
            device_id_type=MESH,
        )

    @pl.loop(1, LINES)
    def _(k):
        share(k).start()

    for c in range(2):

        @pl.loop(1, LINES)
        def _(k, c=c):
            direct(c, k).wait_send()

            @pl.when(lax.rem(me + k, 2) == 1)
            def _():
                margin(c, k).wait_send()

        @pl.when(odd)
        def _(c=c):
            @pl.loop(0, LINES)
            def _(k):
                onward(c, k).wait_send()

    erecv[0] = energy

    @pl.loop(1, LINES)
    def _(k):
        share(k).wait_recv()

    total = jnp.sum(jnp.sum(erecv[...], axis=0), axis=(0, 1), keepdims=True)
    scale = lax.rsqrt(total / (RKEEP * AZ) + 1e-06)

    @pl.loop(0, 32)
    def _(m):
        for comp in range(2):
            v = img[pl.ds(32 * comp + m, ROWS, stride=PITCH), :]
            at = pl.ds(pl.multiple_of(128 * m, 128), 128)
            out_ref[0, comp, :, at] = (v * scale).astype(BF16)

    @pl.loop(1, LINES)
    def _(k):
        share(k).wait_send()


def local(echoes, range_filter, rcmc_weights, fm_rate, rcmc_shift, seam_width, seam_link):
    import functools

    vmem = pl.BlockSpec(memory_space=pltpu.VMEM)
    smem = pl.BlockSpec(memory_space=pltpu.SMEM)
    hbm = pl.BlockSpec(memory_space=pltpu.HBM)
    dma = pltpu.SemaphoreType.DMA
    image = pl.pallas_call(
        functools.partial(kernel, lax.axis_size("chip")),
        out_shape=jax.ShapeDtypeStruct((1, 2, ROWS, AZ), BF16),
        in_specs=[hbm] * 5 + [smem] * 2 + [hbm] * 8,
        out_specs=vmem,
        scratch_shapes=[
            pltpu.VMEM((2, 4096), F32),
            pltpu.VMEM((TAPS, 4096), F32),
            pltpu.SMEM((1, ROWS), F32),
            pltpu.SMEM((1, ROWS), jnp.int32),
            pltpu.VMEM((64, 64), F32),
            pltpu.VMEM((2, 32, 128), F32),
            pltpu.VMEM((256, 256), F32),
            pltpu.VMEM((64, 192), BF16),
            pltpu.VMEM((2, 32, 128), F32),
            pltpu.VMEM((768, 256), BF16),
            pltpu.VMEM((768, 256), BF16),
            pltpu.VMEM((80, 192), BF16),
            pltpu.VMEM((2, 256, 4096), BF16),
            pltpu.VMEM((64, 128), F32),
            pltpu.VMEM((80, 128), F32),
            pltpu.VMEM((4, 35 * 128, 128), BF16),
            pltpu.VMEM((RKEEP, 256), F32),
            pltpu.VMEM((2, 48 * LINES + 40, 128), F32),
            pltpu.VMEM((2 * LINES * SLOT, 128), F32),
            pltpu.VMEM((32 * TAPS, 128), F32),
            pltpu.VMEM((TAPS, 32, 128), F32),
            pltpu.VMEM((32 * NEED, 256), BF16),
            pltpu.VMEM((32 * NEED, 256), BF16),
            pltpu.VMEM((NEED, 32, 256), F32),
            pltpu.VMEM((ROWS, 32, 128), F32),
            pltpu.VMEM((ROWS, 32, 128), F32),
            pltpu.VMEM((32 * ROWS, 256), BF16),
            pltpu.VMEM((32 * ROWS, 256), BF16),
            pltpu.VMEM((32 * ROWS, 256), F32),
            pltpu.VMEM((PITCH * ROWS, 128), F32),
            pltpu.VMEM((2 * ROWS, 128), F32),
            pltpu.VMEM((2 * ROWS, 128), F32),
            pltpu.VMEM((8, 128), F32),
            pltpu.VMEM((LINES, 8, 128), F32),
            dma((12,)),
            dma((2,)),
            dma((2, LINES)),
            dma((2, LINES)),
            dma((2, LINES)),
            dma((2, LINES)),
            dma((2, LINES)),
            dma((2,)),
            dma((LINES,)),
            dma((LINES,)),
        ],
        compiler_params=pltpu.CompilerParams(
            collective_id=0, has_side_effects=True, vmem_limit_bytes=67_043_328
        ),
        name="focus",
    )(
        echoes,
        range_filter,
        rcmc_weights,
        fm_rate,
        rcmc_shift,
        seam_width,
        seam_link,
        *(jnp.asarray(t) for t in tables()),
    )
    return image


def solution(mesh):
    in_specs = (
        P("chip", None, "line", None),
        P(),
        P(),
        P("chip", "line"),
        P("chip", "line"),
        P("chip"),
        P("chip"),
    )
    out_specs = P("chip", None, "line", None)
    return jax.shard_map(local, mesh=mesh, in_specs=in_specs, out_specs=out_specs, check_vma=False)
```
